256 devices in a mesh: grp: 4 (over x), mem: 64 (over z, y, core).
Axes of the slice: x: 4, y: 4, z: 8, core: 2. Of those that a mesh axis runs over, the one named last changes fastest.
Arguments:
- background_tensor: bfloat16 [512, 256, 1024], P('grp', 'mem'), may hold values from -6 to 6
- reading_tally: int32 [512], P(('grp', 'mem')), may hold values from 128 to 1024, as said below
- measurement_slot: int32 [512, 1024], P(('grp', 'mem')), may hold values from 0 to 1023
- reading_datum: float32 [512, 1024], P(('grp', 'mem')), may hold values from -6 to 6
- error_precision: float32 [512, 1024], P(('grp', 'mem')), may hold values from 0.5 to 16
- reading_offset: float32 [512, 1024], P(('grp', 'mem')), may hold values from 0 to 1
Outputs:
- analysis: bfloat16 [512, 256, 1024], P('grp', 'mem')
The draws below stay inside these ranges and needn't reach their ends.
Inputs may be any that keep to these rules, and one draw needn't show every extreme that they name: `reading_tally`: each column's live observations fill its first slots; at least one column has exactly 1024.
All inputs are finite; a program needn't handle non-finite values.
Results may differ from the reference program's by a relative error of at most 0.0074.
Values may be sent and summed in bfloat16 or wider, within the bound.
No kernel may reach another device: no remote copies, remote signals or barrier semaphores. Data moves between devices by JAX's collectives and lax.ppermute only.
A program may use at most 64 MiB of HBM per device.

```python
import math
import jax
import jax.numpy as jnp
from jax import lax

MEMBER_NUMBER = 256
COLUMN_SIZE_VERT = 1024
MAXOBS = 1024
NSTEPS = 5
DOMAIN_SITES = 512


def draw_reading_tally(key, part):
    first, second, third = jax.random.split(jax.random.fold_in(key, 17), 3)
    level = jax.random.randint(first, (DOMAIN_SITES,), 0, 3)
    base = jnp.left_shift(jnp.full((DOMAIN_SITES,), MAXOBS // 8, jnp.int32), level)
    extra = jax.random.randint(second, (DOMAIN_SITES,), 0, 1048576) % base
    chosen = jax.random.randint(third, (), 0, DOMAIN_SITES)
    counts = jnp.where(jnp.arange(DOMAIN_SITES, dtype=jnp.int32) == chosen, MAXOBS, base + extra)
    return counts.astype(jnp.int32)


def set_ends(values, own_key, smallest, largest):
    longest = values.shape.index(max(values.shape))
    spots = []
    for shift in (0, 1):
        where = [jax.random.randint(jax.random.fold_in(own_key, axis), (), 0, length) for axis, length in enumerate(values.shape)]
        where[longest] = (where[longest] + shift) % values.shape[longest]
        spots.append(tuple(where))
    return values.at[spots[0]].set(smallest).at[spots[1]].set(largest)


def levels(own_key, shape, pieces, smallest, high):
    gain = 1.0
    for position, shards_of in pieces:
        draws = jax.random.uniform(jax.random.fold_in(jax.random.fold_in(own_key, 6), position), (shards_of,), jnp.float32, smallest / len(pieces), high / len(pieces))
        gain = gain * jnp.repeat(jnp.exp(draws), shape[position] // shards_of).reshape((-1,) + (1,) * (len(shape) - 1 - position))
    return gain


def scatter_about(rng, dims, width, reach, cuts=(), kind=jnp.bfloat16):
    values = width * jax.random.normal(rng, dims, jnp.float32)
    if cuts:
        values = values * levels(rng, dims, cuts, -0.22, 0.18)
    return jnp.clip(values, -reach, reach).astype(kind)


def setup_inputs(seed: int = 0) -> dict:
    splits = jax.random.split(jax.random.key(seed), 7)
    background_tensor = scatter_about(splits[0], (DOMAIN_SITES, MEMBER_NUMBER, COLUMN_SIZE_VERT), 1.0, 6.0, ((0, 4), (1, 64)))
    reading_tally = draw_reading_tally(jax.random.fold_in(splits[6], 71), 0)
    measurement_slot = set_ends(jax.random.randint(splits[2], (DOMAIN_SITES, MAXOBS), 0, COLUMN_SIZE_VERT), jax.random.fold_in(splits[2], 1), 0, COLUMN_SIZE_VERT - 1).astype(jnp.int32)
    reading_datum = scatter_about(splits[3], (DOMAIN_SITES, MAXOBS), 1.0, 6.0, ((0, 256),), jnp.float32)
    error_precision = jnp.clip(jnp.exp(math.log(16.0) - 3.465736 * jax.random.uniform(splits[4], (DOMAIN_SITES, MAXOBS), jnp.float32) ** levels(splits[4], (DOMAIN_SITES, MAXOBS), ((0, 256),), -0.2, 0.2)), 0.5, 16.0)
    reading_offset = jnp.clip(1.0 * jax.random.uniform(splits[5], (DOMAIN_SITES, MAXOBS), jnp.float32) ** levels(splits[5], (DOMAIN_SITES, MAXOBS), ((0, 256),), -0.2, 0.2), 0.0, 1.0)
    return dict(background_tensor=background_tensor, reading_tally=reading_tally, measurement_slot=measurement_slot, reading_datum=reading_datum, error_precision=error_precision, reading_offset=reading_offset)


def direction_weights(shift_amount):
    toward_west = jnp.exp(-(shift_amount + 0.5) ** 2)
    own_weight = jnp.exp(-(shift_amount - 0.5) ** 2)
    toward_east = jnp.exp(-(1.5 - shift_amount) ** 2)
    return (toward_west, own_weight, toward_east)

def local_summary(background_members):
    sample_slices = background_members.shape[0]
    model_vector32 = background_members.astype(jnp.float32)
    focal_site = lax.optimization_barrier(jnp.sum(model_vector32, axis=0)) / sample_slices
    anomaly_matrix = (model_vector32 - focal_site[None, :]).astype(jnp.bfloat16)
    return (focal_site, anomaly_matrix)

def local_measurements(background_members, position_number, quantity, scalar_amount, noise_weighting, shift_amount, lateral_neighbor):
    focal_site, anomaly_matrix = local_summary(background_members)
    obs_slots = position_number.shape[0]
    measured_vector = jnp.take(anomaly_matrix, position_number, axis=1)
    innovation = scalar_amount - jnp.take(focal_site, position_number, axis=0)
    live_mask = (jnp.arange(obs_slots, dtype=jnp.int32) < quantity).astype(jnp.float32)
    weight = direction_weights(shift_amount)[lateral_neighbor]
    factor = jnp.sqrt(weight * noise_weighting) * live_mask
    scaled = (measured_vector.astype(jnp.float32) * factor[None, :]).astype(jnp.bfloat16)
    shifted = (innovation * factor).astype(jnp.bfloat16)
    padding = jnp.zeros((7, obs_slots), jnp.bfloat16)
    obs_rows = jnp.concatenate([scaled, shifted[None, :], padding], axis=0)
    sample_slices = background_members.shape[0]
    return jnp.dot(obs_rows, obs_rows[:sample_slices].T, preferred_element_type=jnp.float32)

def inverse_root(matrix):
    size = matrix.shape[0]
    identity = jnp.eye(size, dtype=jnp.float32)
    norm_value = jnp.sqrt(jnp.sum(matrix * matrix))
    iterate = matrix / norm_value
    inverse = identity
    for iteration in range(NSTEPS):
        middle = 1.5 * identity - 0.5 * jnp.dot(inverse, iterate, precision=lax.Precision.HIGHEST)
        iterate = jnp.dot(iterate, middle, precision=lax.Precision.HIGHEST)
        inverse = jnp.dot(middle, inverse, precision=lax.Precision.HIGHEST)
    return inverse / jnp.sqrt(norm_value)

def reference(background_tensor, reading_tally, measurement_slot, reading_datum, error_precision, reading_offset):
    vertical_slices = background_tensor.shape[0]
    sample_slices = background_tensor.shape[1]

    def chosen_sample(array, vertical_slice):
        return lax.dynamic_index_in_dim(array, vertical_slice, 0, keepdims=False)

    def gram_of(vertical_slice, lateral_neighbor):
        return local_measurements(chosen_sample(background_tensor, vertical_slice), chosen_sample(measurement_slot, vertical_slice), chosen_sample(reading_tally, vertical_slice), chosen_sample(reading_datum, vertical_slice), chosen_sample(error_precision, vertical_slice), chosen_sample(reading_offset, vertical_slice), lateral_neighbor)

    def analyse(vertical_slice):
        western = (vertical_slice + vertical_slices - 1) % vertical_slices
        eastern = (vertical_slice + 1) % vertical_slices
        combined = gram_of(vertical_slice, 1) + gram_of(western, 2) + gram_of(eastern, 0)
        focal_site, anomaly_matrix = local_summary(chosen_sample(background_tensor, vertical_slice))
        identity = jnp.eye(sample_slices, dtype=jnp.float32)
        system = (sample_slices - 1) * identity + combined[:sample_slices]
        pull_vec = combined[sample_slices]
        inv_root = inverse_root(system)
        mean_weight = jnp.dot(inv_root, jnp.dot(inv_root, pull_vec, precision=lax.Precision.HIGHEST), precision=lax.Precision.HIGHEST)
        weight_matrix = (jnp.sqrt(sample_slices - 1.0) * inv_root + mean_weight[:, None]).astype(jnp.bfloat16)
        increment = jnp.dot(weight_matrix.T, anomaly_matrix, preferred_element_type=jnp.float32)
        return (focal_site[None, :] + increment).astype(jnp.bfloat16)
    return lax.map(analyse, jnp.arange(vertical_slices, dtype=jnp.int32))
```

```python
import jax
import jax.numpy as jnp
from jax import lax
from jax.sharding import PartitionSpec as P

NSTEPS = 5
HIGH = lax.Precision.HIGH
HIGHEST = lax.Precision.HIGHEST


def direction_weights(shift_amount):
    toward_west = jnp.exp(-((shift_amount + 0.5) ** 2))
    own_weight = jnp.exp(-((shift_amount - 0.5) ** 2))
    toward_east = jnp.exp(-((1.5 - shift_amount) ** 2))
    return (toward_west, own_weight, toward_east)


def binned(tally, slot, datum, precision, offset, values):
    slots = slot.shape[0]
    live = (jnp.arange(slots, dtype=jnp.int32) < tally).astype(jnp.float32)
    weights = jnp.stack(direction_weights(offset)) * (precision * live)[None]
    rows = jnp.concatenate([weights, weights * datum[None]], axis=0)
    chosen = (slot[:, None] == jnp.arange(values, dtype=jnp.int32)[None, :]).astype(jnp.float32)
    return jnp.dot(rows, chosen, precision=HIGHEST)


def summary(members):
    wide = members.astype(jnp.float32)
    center = jnp.sum(wide, axis=0) / members.shape[0]
    return center, (wide - center[None]).astype(jnp.bfloat16)


def products(center, spread, bins, which):
    weight, driven = bins[which], bins[3 + which]
    rows = (spread.astype(jnp.float32) * jnp.sqrt(weight)[None]).astype(jnp.bfloat16)
    gram = lax.dot_general(
        rows, rows, (((1,), (1,)), ((), ())), preferred_element_type=jnp.float32
    )
    drive = driven - weight * center
    pull = lax.dot_general(
        jnp.broadcast_to(drive[None], (8, drive.shape[0])),
        spread.astype(jnp.float32),
        (((1,), (1,)), ((), ())),
        precision=HIGH,
    )
    return jnp.concatenate([gram, pull], axis=0)


def transform_of(combined):
    count = combined.shape[1]
    eye = jnp.eye(count, dtype=jnp.float32)
    system = (count - 1) * eye + combined[:count]
    pull = combined[count]
    norm = jnp.sqrt(jnp.sum(system * system))
    iterate = system / norm
    inverse = 1.5 * eye - 0.5 * iterate
    iterate = jnp.dot(iterate, inverse, precision=HIGH)
    for step in range(1, NSTEPS):
        middle = 1.5 * eye - 0.5 * jnp.dot(inverse, iterate, precision=HIGH)
        if step < NSTEPS - 1:
            iterate = jnp.dot(iterate, middle, precision=HIGH)
        inverse = jnp.dot(middle, inverse, precision=HIGH)
    root = inverse / jnp.sqrt(norm)
    inner = jnp.dot(root, pull, precision=HIGHEST)
    mean_weight = jnp.dot(root, inner, precision=HIGHEST)
    return (jnp.sqrt(count - 1.0) * root + mean_weight[:, None]).astype(jnp.bfloat16)


def analysed(center, spread, transform):
    grown = lax.dot_general(
        transform, spread, (((0,), (0,)), ((), ())), preferred_element_type=jnp.float32
    )
    return (center[None] + grown).astype(jnp.bfloat16)


def exchange(value):
    return lax.all_to_all(value, "mem", split_axis=0, concat_axis=0, tiled=True)


def per_device(background, tally, slot, datum, precision, offset):
    columns, held, values = background.shape
    sides = background.reshape(columns // 2, 2, held, values)
    even_in = exchange(sides[:, 0])
    odd_in = exchange(sides[:, 1])
    bins = [
        binned(tally[c], slot[c], datum[c], precision[c], offset[c], values) for c in range(2)
    ]
    count = lax.axis_size("grp") * lax.axis_size("mem")
    up = [(i, (i + 1) % count) for i in range(count)]
    down = [(b, a) for a, b in up]
    even_in = even_in.reshape(-1, values)
    odd_in = odd_in.reshape(-1, values)
    even_center, even_spread = summary(even_in)
    from_east = lax.ppermute(products(even_center, even_spread, bins[0], 0), ("grp", "mem"), down)
    even_own = products(even_center, even_spread, bins[0], 1)
    even_east = products(even_center, even_spread, bins[0], 2)

    odd_center, odd_spread = summary(odd_in)
    from_west = lax.ppermute(products(odd_center, odd_spread, bins[1], 2), ("grp", "mem"), up)
    odd_own = products(odd_center, odd_spread, bins[1], 1)
    odd_west = products(odd_center, odd_spread, bins[1], 0)

    odd_out = analysed(odd_center, odd_spread, transform_of(odd_own + even_east + from_east))
    odd_out = exchange(odd_out.reshape(columns // 2, held, values))
    even_out = analysed(even_center, even_spread, transform_of(even_own + from_west + odd_west))
    even_out = exchange(even_out.reshape(columns // 2, held, values))
    return jnp.stack([even_out, odd_out], axis=1).reshape(columns, held, values)


def solution(mesh):
    both = ("grp", "mem")
    in_specs = (
        P("grp", "mem", None),
        P(both),
        P(both, None),
        P(both, None),
        P(both, None),
        P(both, None),
    )
    return jax.shard_map(
        per_device, mesh=mesh, in_specs=in_specs, out_specs=P("grp", "mem", None), check_vma=False
    )
```

```python
import jax
import jax.numpy as jnp
from jax import lax
from jax.experimental import pallas as pl
from jax.experimental.pallas import tpu as pltpu
from jax.sharding import PartitionSpec as P

NSTEPS = 5
HIGHEST = lax.Precision.HIGHEST
F32 = jnp.float32
BF16 = jnp.bfloat16


def direction_weights(shift_amount):
    toward_west = jnp.exp(-((shift_amount + 0.5) ** 2))
    own_weight = jnp.exp(-((shift_amount - 0.5) ** 2))
    toward_east = jnp.exp(-((1.5 - shift_amount) ** 2))
    return (toward_west, own_weight, toward_east)


def binned(tally, slot, datum, precision, offset, values):
    slots = slot.shape[0]
    live = (jnp.arange(slots, dtype=jnp.int32) < tally).astype(F32)
    weights = jnp.stack(direction_weights(offset)) * (precision * live)[None]
    rows = jnp.concatenate([weights, weights * datum[None]], axis=0)
    chosen = (slot[:, None] == jnp.arange(values, dtype=jnp.int32)[None, :]).astype(F32)
    return jnp.dot(rows, chosen, precision=HIGHEST)


def halves(value):
    high = value.astype(BF16)
    return high, (value - high.astype(F32)).astype(BF16)


def product(left, right):
    (left_high, left_low), (right_high, right_low) = left, right
    return jnp.dot(
        jnp.concatenate([left_high, left_high, left_low], axis=1),
        jnp.concatenate([right_high, right_low, right_high], axis=0),
        preferred_element_type=F32,
    )


def against(left, right):
    return lax.dot_general(left, right, (((1,), (1,)), ((), ())), preferred_element_type=F32)


def rows_of(spread, bins, which):
    return (spread.astype(F32) * jnp.sqrt(bins[which : which + 1])).astype(BF16)


def pulls_of(spread, center, bins):
    high, low = halves(bins[3:6] - bins[0:3] * center)
    both = against(jnp.concatenate([high, low], axis=0), spread)
    return both[0:3] + both[3:6]


def outgoing_body(members_ref, bins_ref, spread_ref, center_ref, pulls_ref, west_ref, east_ref):
    peers, _, held, values = members_ref.shape
    count = peers * held
    for column, which, sent in ((0, 0, west_ref), (1, 2, east_ref)):
        wide = members_ref[:, column].astype(F32).reshape(count, values)
        center = jnp.sum(wide, axis=0, keepdims=True) * (1.0 / count)
        center_ref[column : column + 1, :] = center
        spread = (wide - center).astype(BF16)
        spread_ref[column] = spread
        bins = bins_ref[column]
        rows = rows_of(spread, bins, which)
        sent[0:count, :] = against(rows, rows).astype(BF16)
        pulls = pulls_of(spread, center, bins)
        pulls_ref[column] = pulls
        high, low = halves(pulls[which : which + 1])
        sent[count:, :] = jnp.concatenate([high, low, jnp.zeros((14, count), BF16)], axis=0)


def local_body(spread_ref, bins_ref, system_ref):
    count = spread_ref.shape[1]
    for column, other, which in ((0, 1, 0), (1, 0, 2)):
        own = rows_of(spread_ref[column], bins_ref[column], 1)
        side = rows_of(spread_ref[other], bins_ref[other], which)
        rows = jnp.concatenate([own, side], axis=1)
        system_ref[column] = against(rows, rows)


def analysis_body(
    system_ref, pulls_ref, from_west_ref, from_east_ref, spread_ref, center_ref, out_ref
):
    peers, _, held, values = out_ref.shape
    count = peers * held
    diagonal = lax.broadcasted_iota(jnp.int32, (count, count), 0) == lax.broadcasted_iota(
        jnp.int32, (count, count), 1
    )
    half_more = jnp.where(diagonal, 1.5, 0.0).astype(F32)
    eye = jnp.where(diagonal, count - 1.0, 0.0).astype(F32)
    columns = (0, 1)
    iterates, inverses, norms = [], [], []
    for column in columns:
        received = (from_west_ref, from_east_ref)[column]
        system = eye + system_ref[column] + received[0:count, :].astype(F32)
        squares = jnp.sum(jnp.sum(system * system, axis=0, keepdims=True), axis=1, keepdims=True)
        norm = jnp.sqrt(squares)
        iterate = system * (1.0 / norm)
        inverse = halves(half_more - 0.5 * iterate)
        norms.append(norm)
        inverses.append(inverse)
        iterates.append(halves(product(halves(iterate), inverse)))
    roots = [None, None]
    for step in range(1, NSTEPS):
        middles = [
            halves(half_more - 0.5 * product(inverses[column], iterates[column]))
            for column in columns
        ]
        if step < NSTEPS - 1:
            iterates = [halves(product(iterates[column], middles[column])) for column in columns]
        roots = [product(middles[column], inverses[column]) for column in columns]
        inverses = [halves(root) for root in roots]
    for column in columns:
        received = (from_west_ref, from_east_ref)[column]
        arrived = received[count:, :].astype(F32)
        pulls, others = pulls_ref[column], pulls_ref[1 - column]
        side = (0, 2)[column]
        pull = pulls[1:2] + others[side : side + 1] + arrived[0:1] + arrived[1:2]
        root = roots[column] * (1.0 / jnp.sqrt(norms[column]))
        inner = jnp.sum(root * pull, axis=1, keepdims=True)
        mean_weight = jnp.sum(root * inner, axis=0, keepdims=True)
        transform = ((count - 1.0) ** 0.5 * root + mean_weight).astype(BF16)
        grown = jnp.dot(transform, spread_ref[column], preferred_element_type=F32)
        analysis = center_ref[column : column + 1, :] + grown
        out_ref[:, column] = analysis.reshape(peers, held, values).astype(BF16)


def call(body, flops, outs, *operands):
    return pl.pallas_call(
        body,
        out_shape=outs,
        in_specs=[pl.BlockSpec(memory_space=pltpu.VMEM)] * len(operands),
        out_specs=jax.tree.map(lambda _: pl.BlockSpec(memory_space=pltpu.VMEM), outs),
        compiler_params=pltpu.CompilerParams(vmem_limit_bytes=24 << 20),
        cost_estimate=pl.CostEstimate(flops=flops, bytes_accessed=1 << 20, transcendentals=0),
    )(*operands)


def exchange(value):
    return lax.all_to_all(value, "mem", split_axis=0, concat_axis=0, tiled=True)


def per_device(background, tally, slot, datum, precision, offset):
    columns, held, values = background.shape
    peers = lax.axis_size("mem")
    count = peers * held
    members = exchange(background).reshape(peers, 2, held, values)
    bins = jnp.stack(
        [binned(tally[c], slot[c], datum[c], precision[c], offset[c], values) for c in range(2)]
    )
    shape = jax.ShapeDtypeStruct
    sent = shape((count + 16, count), BF16)
    flops = 2 * count * count * values
    spread, center, pulls, westward, eastward = call(
        outgoing_body,
        2 * flops,
        (
            shape((2, count, values), BF16),
            shape((2, values), F32),
            shape((2, 3, count), F32),
            sent,
            sent,
        ),
        members,
        bins,
    )
    total = lax.axis_size("grp") * peers
    up = [(i, (i + 1) % total) for i in range(total)]
    from_west = lax.ppermute(eastward, ("grp", "mem"), up)
    from_east = lax.ppermute(westward, ("grp", "mem"), [(b, a) for a, b in up])
    system = call(local_body, 4 * flops, shape((2, count, count), F32), spread, bins)
    analysis = call(
        analysis_body,
        2 * flops + 2 * 12 * 3 * 2 * count**3,
        shape((peers, 2, held, values), BF16),
        system,
        pulls,
        from_west,
        from_east,
        spread,
        center,
    )
    return exchange(analysis.reshape(columns, held, values))


def solution(mesh):
    both = ("grp", "mem")
    in_specs = (
        P("grp", "mem", None),
        P(both),
        P(both, None),
        P(both, None),
        P(both, None),
        P(both, None),
    )
    return jax.shard_map(
        per_device, mesh=mesh, in_specs=in_specs, out_specs=P("grp", "mem", None), check_vma=False
    )
```

```python
import jax
import jax.numpy as jnp
import numpy as np
from jax import lax
from jax.experimental import pallas as pl
from jax.experimental.pallas import tpu as pltpu
from jax.sharding import PartitionSpec as P


BOTH = ("grp", "mem")
HIGHEST = lax.Precision.HIGHEST
F32 = jnp.float32
BF16 = jnp.bfloat16


def direction_weights(shift_amount):
    toward_west = jnp.exp(-((shift_amount + 0.5) ** 2))
    own_weight = jnp.exp(-((shift_amount - 0.5) ** 2))
    toward_east = jnp.exp(-((1.5 - shift_amount) ** 2))
    return (toward_west, own_weight, toward_east)


def binned(observations, values):
    slot, datum, precision, offset = observations
    weights = jnp.stack(direction_weights(offset)) * precision[None]
    rows = jnp.concatenate([weights, weights * datum[None]], axis=0)
    picks = slot.astype(jnp.int32)
    chosen = (picks[:, None] == jnp.arange(values, dtype=jnp.int32)[None, :]).astype(F32)
    return jnp.dot(rows, chosen, precision=HIGHEST)


def walk():
    chips = [row * 4 + (place, 3 - place)[row % 2] for row in range(8) for place in range(4)]
    return [0] + [2 * chip + core for chip in chips[1:] for core in (0, 1)] + [1]


def two_step_factors():
    root = max(np.roots([1.0, -6.0, 9.0, -12.0]), key=np.real).real
    return (-(3.0 + root) / 4, 3.0 * root / 4), ((root - 6.0) / 4, 3.0 / root)


def halves(value):
    high = value.astype(BF16)
    return high, (value - high.astype(F32)).astype(BF16)


def product(left, right):
    (left_high, left_low), (right_high, right_low) = left, right
    return jnp.dot(
        jnp.concatenate([left_high, left_high, left_low], axis=1),
        jnp.concatenate([right_high, right_low, right_high], axis=0),
        preferred_element_type=F32,
    )


def against(left, right):
    return lax.dot_general(left, right, (((1,), (1,)), ((), ())), preferred_element_type=F32)


def rows_of(spread, bins, which):
    return (spread.astype(F32) * jnp.sqrt(bins[which : which + 1])).astype(BF16)


def pulls_of(spread, center, bins):
    high, low = halves(bins[3:6] - bins[0:3] * center)
    both = against(jnp.concatenate([high, low], axis=0), spread)
    return both[0:3] + both[3:6]


def outgoing_body(members_ref, bins_ref, spread_ref, center_ref, pulls_ref, west_ref, east_ref):
    peers, _, held, values = members_ref.shape
    count = peers * held
    for column, which, sent in ((0, 0, west_ref), (1, 2, east_ref)):
        wide = members_ref[:, column].astype(F32).reshape(count, values)
        center = jnp.sum(wide, axis=0, keepdims=True) * (1.0 / count)
        center_ref[column : column + 1, :] = center
        spread = (wide - center).astype(BF16)
        spread_ref[column] = spread
        bins = bins_ref[column]
        rows = rows_of(spread, bins, which)
        sent[0:count, :] = against(rows, rows).astype(BF16)
        pulls = pulls_of(spread, center, bins)
        pulls_ref[column] = pulls
        high, low = halves(pulls[which : which + 1])
        sent[count:, :] = jnp.concatenate([high, low, jnp.zeros((14, count), BF16)], axis=0)


def local_body(spread_ref, bins_ref, system_ref):
    for column, other, which in ((0, 1, 0), (1, 0, 2)):
        own = rows_of(spread_ref[column], bins_ref[column], 1)
        side = rows_of(spread_ref[other], bins_ref[other], which)
        rows = jnp.concatenate([own, side], axis=1)
        system_ref[column] = against(rows, rows)


def analysis_body(
    system_ref, pulls_ref, from_west_ref, from_east_ref, spread_ref, center_ref, out_ref
):
    peers, _, held, values = out_ref.shape
    count = peers * held
    diagonal = lax.broadcasted_iota(jnp.int32, (count, count), 0) == lax.broadcasted_iota(
        jnp.int32, (count, count), 1
    )

    def scaled_eye(value):
        return jnp.where(diagonal, value, 0.0).astype(F32)

    columns = (0, 1)
    quadratics = [(linear, scaled_eye(constant)) for linear, constant in two_step_factors()]

    def two_steps(ratios):
        split = [halves(ratio) for ratio in ratios]
        squares = [0.25 * product(x, x) for x in split]
        factors = [
            [halves(square + linear * ratio + constant) for linear, constant in quadratics]
            for square, ratio in zip(squares, ratios)
        ]
        return split, [halves(product(*pair)) for pair in factors]

    def advanced(split, gains):
        twice = [halves(product(gain, gain)) for gain in gains]
        return [product(x, gain) for x, gain in zip(split, twice)]

    norms, ratios = [], []
    for column in columns:
        received = (from_west_ref, from_east_ref)[column]
        system = scaled_eye(count - 1.0) + system_ref[column] + received[0:count, :].astype(F32)
        squares = jnp.sum(jnp.sum(system * system, axis=0, keepdims=True), axis=1, keepdims=True)
        norm = jnp.sqrt(squares)
        norms.append(norm)
        ratios.append(system * (1.0 / norm))
    split, first = two_steps(ratios)
    ratios = advanced(split, first)
    split, second = two_steps(ratios)
    inverses = [halves(product(*pair)) for pair in zip(first, second)]
    ratios = advanced(split, second)
    half_more = scaled_eye(1.5)
    roots = [
        product(halves(half_more - 0.5 * ratio), inverse)
        for ratio, inverse in zip(ratios, inverses)
    ]
    for column in columns:
        received = (from_west_ref, from_east_ref)[column]
        arrived = received[count:, :].astype(F32)
        pulls, others = pulls_ref[column], pulls_ref[1 - column]
        side = (0, 2)[column]
        pull = pulls[1:2] + others[side : side + 1] + arrived[0:1] + arrived[1:2]
        root = roots[column] * (1.0 / jnp.sqrt(norms[column]))
        inner = jnp.sum(root * pull, axis=1, keepdims=True)
        mean_weight = jnp.sum(root * inner, axis=0, keepdims=True)
        transform = ((count - 1.0) ** 0.5 * root + mean_weight).astype(BF16)
        grown = jnp.dot(transform, spread_ref[column], preferred_element_type=F32)
        analysis = center_ref[column : column + 1, :] + grown
        out_ref[:, column] = analysis.reshape(peers, held, values).astype(BF16)


def call(body, flops, outs, *operands):
    return pl.pallas_call(
        body,
        out_shape=outs,
        in_specs=[pl.BlockSpec(memory_space=pltpu.VMEM)] * len(operands),
        out_specs=jax.tree.map(lambda _: pl.BlockSpec(memory_space=pltpu.VMEM), outs),
        compiler_params=pltpu.CompilerParams(vmem_limit_bytes=24 << 20),
        cost_estimate=pl.CostEstimate(flops=flops, bytes_accessed=1 << 20, transcendentals=0),
    )(*operands)


def exchange(value):
    return lax.all_to_all(
        value, "mem", split_axis=0, concat_axis=0, tiled=True, axis_index_groups=[walk()]
    )


def analyse(background, tally, slot, datum, precision, offset):
    columns, held, values = background.shape
    peers, groups = lax.axis_size("mem"), lax.axis_size("grp")
    count = peers * held
    order = walk()
    members = exchange(background).reshape(peers, 2, held, values)
    live = jnp.arange(values, dtype=jnp.int32)[None, :] < tally[:, None]
    observations = jnp.stack(
        [slot.astype(F32), datum, precision * live.astype(F32), offset], axis=0
    )
    observations = lax.ppermute(
        observations.reshape(8, values), "mem", [(p, order[p]) for p in range(peers)]
    ).reshape(4, 2, values)
    bins = jnp.stack([binned(observations[:, c], values) for c in range(2)])
    shape = jax.ShapeDtypeStruct
    sent = shape((count + 16, count), BF16)
    flops = 2 * count * count * values
    spread, center, pulls, westward, eastward = call(
        outgoing_body,
        2 * flops,
        (
            shape((2, count, values), BF16),
            shape((2, values), F32),
            shape((2, 3, count), F32),
            sent,
            sent,
        ),
        members,
        bins,
    )
    ring = [group * peers + place for group in range(groups) for place in order]
    up = list(zip(ring, ring[1:] + ring[:1]))
    from_west = lax.ppermute(eastward, BOTH, up)
    from_east = lax.ppermute(westward, BOTH, [(b, a) for a, b in up])
    system = call(local_body, 4 * flops, shape((2, count, count), F32), spread, bins)
    analysis = call(
        analysis_body,
        2 * flops + 2 * 10 * 3 * 2 * count**3,
        shape((peers, 2, held, values), BF16),
        system,
        pulls,
        from_west,
        from_east,
        spread,
        center,
    )
    return exchange(analysis.reshape(columns, held, values))


def solution(mesh):
    in_specs = (
        P("grp", "mem", None),
        P(BOTH),
        P(BOTH, None),
        P(BOTH, None),
        P(BOTH, None),
        P(BOTH, None),
    )
    return jax.shard_map(
        analyse, mesh=mesh, in_specs=in_specs, out_specs=P("grp", "mem", None), check_vma=False
    )
```

```python
import jax
import jax.numpy as jnp
import numpy as np
from jax import lax
from jax.experimental import pallas as pl
from jax.experimental.pallas import tpu as pltpu
from jax.sharding import PartitionSpec as P


BOTH = ("grp", "mem")
HIGHEST = lax.Precision.HIGHEST
F32 = jnp.float32
BF16 = jnp.bfloat16


def direction_weights(shift_amount):
    toward_west = jnp.exp(-((shift_amount + 0.5) ** 2))
    own_weight = jnp.exp(-((shift_amount - 0.5) ** 2))
    toward_east = jnp.exp(-((1.5 - shift_amount) ** 2))
    return (toward_west, own_weight, toward_east)


def binned(observations, values):
    slot, datum, precision, offset = observations
    weights = jnp.stack(direction_weights(offset)) * precision[None]
    rows = jnp.concatenate([weights, weights * datum[None]], axis=0)
    picks = slot.astype(jnp.int32)
    chosen = (picks[:, None] == jnp.arange(values, dtype=jnp.int32)[None, :]).astype(F32)
    return jnp.dot(rows, chosen, precision=HIGHEST)


def walk():
    chips = [row * 4 + (place, 3 - place)[row % 2] for row in range(8) for place in range(4)]
    return [2 * chip + core for chip in chips for core in (0, 1)]


def two_step_factors():
    root = max(np.roots([1.0, -6.0, 9.0, -12.0]), key=np.real).real
    return (-(3.0 + root) / 4, 3.0 * root / 4), ((root - 6.0) / 4, 3.0 / root)


def halves(value):
    high = value.astype(BF16)
    return high, (value - high.astype(F32)).astype(BF16)


def product(left, right):
    (left_high, left_low), (right_high, right_low) = left, right
    return jnp.dot(
        jnp.concatenate([left_high, left_high, left_low], axis=1),
        jnp.concatenate([right_high, right_low, right_high], axis=0),
        preferred_element_type=F32,
    )


def against(left, right):
    return lax.dot_general(left, right, (((1,), (1,)), ((), ())), preferred_element_type=F32)


def rows_of(spread, bins, which):
    return (spread.astype(F32) * jnp.sqrt(bins[which : which + 1])).astype(BF16)


def pulls_of(spread, center, bins):
    high, low = halves(bins[3:6] - bins[0:3] * center)
    both = against(jnp.concatenate([high, low], axis=0), spread)
    return both[0:3] + both[3:6]


def outgoing_body(
    parity_ref, members_ref, bins_ref, spread_ref, center_ref, pulls_ref, chip_ref, next_ref
):
    peers, _, held, values = members_ref.shape
    count = peers * held
    for column in (0, 1):
        wide = members_ref[:, column].astype(F32).reshape(count, values)
        center = jnp.sum(wide, axis=0, keepdims=True) * (1.0 / count)
        center_ref[column] = center
        spread = (wide - center).astype(BF16)
        spread_ref[column] = spread
        pulls_ref[column] = pulls_of(spread, center, bins_ref[column])
    parity = parity_ref[0]
    for column, sent in ((parity, next_ref), (1 - parity, chip_ref)):
        even = column == 0
        bins, pulls = bins_ref[column], pulls_ref[column]
        scale = jnp.sqrt(jnp.where(even, bins[0:1], bins[2:3]))
        rows = (spread_ref[column].astype(F32) * scale).astype(BF16)
        sent[0:count, :] = against(rows, rows).astype(BF16)
        high, low = halves(jnp.where(even, pulls[0:1], pulls[2:3]))
        sent[count:, :] = jnp.concatenate([high, low, jnp.zeros((14, count), BF16)], axis=0)


def local_body(spread_ref, bins_ref, system_ref):
    for column, other, which in ((0, 1, 0), (1, 0, 2)):
        own = rows_of(spread_ref[column], bins_ref[column], 1)
        side = rows_of(spread_ref[other], bins_ref[other], which)
        rows = jnp.concatenate([own, side], axis=1)
        system_ref[column] = against(rows, rows)


def analysis_of(column, system_ref, pulls_ref, received_ref, spread_ref, center_ref, out_ref):
    peers, _, held, values = out_ref.shape
    count = peers * held
    diagonal = lax.broadcasted_iota(jnp.int32, (count, count), 0) == lax.broadcasted_iota(
        jnp.int32, (count, count), 1
    )

    def scaled_eye(value):
        return jnp.where(diagonal, value, 0.0).astype(F32)

    def two_steps(ratio):
        split = halves(ratio)
        square = 0.25 * product(split, split)
        factors = [
            halves(square + linear * ratio + scaled_eye(constant))
            for linear, constant in two_step_factors()
        ]
        return split, halves(product(*factors))

    def advanced(split, gain):
        return product(split, halves(product(gain, gain)))

    system = scaled_eye(count - 1.0) + system_ref[column] + received_ref[0:count, :].astype(F32)
    squares = jnp.sum(jnp.sum(system * system, axis=0, keepdims=True), axis=1, keepdims=True)
    norm = jnp.sqrt(squares)
    split, first = two_steps(system * (1.0 / norm))
    split, second = two_steps(advanced(split, first))
    inverse = halves(product(first, second))
    last = halves(scaled_eye(1.5) - 0.5 * advanced(split, second))
    root = product(last, inverse) * (1.0 / jnp.sqrt(norm))
    arrived = received_ref[count:, :].astype(F32)
    pulls, others = pulls_ref[column], pulls_ref[1 - column]
    side = jnp.where(column == 0, others[0:1], others[2:3])
    pull = pulls[1:2] + side + arrived[0:1] + arrived[1:2]
    inner = jnp.sum(root * pull, axis=1, keepdims=True)
    mean_weight = jnp.sum(root * inner, axis=0, keepdims=True)
    transform = ((count - 1.0) ** 0.5 * root + mean_weight).astype(BF16)
    grown = jnp.dot(transform, spread_ref[column], preferred_element_type=F32)
    analysis = center_ref[column] + grown
    out_ref[:, column] = analysis.reshape(peers, held, values).astype(BF16)


def chip_body(parity_ref, *refs):
    analysis_of(1 - parity_ref[0], *refs)


def next_body(parity_ref, done_ref, *refs):
    analysis_of(parity_ref[0], *refs)


def call(body, flops, outs, *operands, aliases=None):
    return pl.pallas_call(
        body,
        out_shape=outs,
        in_specs=[
            pl.BlockSpec(memory_space=pltpu.SMEM if operand.ndim == 1 else pltpu.VMEM)
            for operand in operands
        ],
        out_specs=jax.tree.map(lambda _: pl.BlockSpec(memory_space=pltpu.VMEM), outs),
        input_output_aliases=aliases or {},
        compiler_params=pltpu.CompilerParams(vmem_limit_bytes=24 << 20),
        cost_estimate=pl.CostEstimate(flops=flops, bytes_accessed=1 << 20, transcendentals=0),
    )(*operands)


def exchange(value):
    return lax.all_to_all(
        value, "mem", split_axis=0, concat_axis=0, tiled=True, axis_index_groups=[walk()]
    )


def analyse(background, tally, slot, datum, precision, offset):
    columns, held, values = background.shape
    peers, groups = lax.axis_size("mem"), lax.axis_size("grp")
    count = peers * held
    order = walk()
    members = exchange(background).reshape(peers, 2, held, values)
    live = jnp.arange(values, dtype=jnp.int32)[None, :] < tally[:, None]
    observations = jnp.stack(
        [slot.astype(F32), datum, precision * live.astype(F32), offset], axis=0
    )
    observations = lax.ppermute(
        observations.reshape(8, values), "mem", [(p, order[p]) for p in range(peers)]
    ).reshape(4, 2, values)
    bins = jnp.stack([binned(observations[:, c], values) for c in range(2)])
    shape = jax.ShapeDtypeStruct
    sent = shape((count + 16, count), BF16)
    flops = 2 * count * count * values
    parity = (lax.axis_index("mem") % 2).astype(jnp.int32)[None]
    spread, center, pulls, to_chip, to_next = call(
        outgoing_body,
        2 * flops,
        (
            shape((2, count, values), BF16),
            shape((2, 1, values), F32),
            shape((2, 3, count), F32),
            sent,
            sent,
        ),
        parity,
        members,
        bins,
    )
    ring = [group * peers + place for group in range(groups) for place in order]
    pairs = [tuple(ring[n : n + 2]) for n in range(0, len(ring), 2)]
    gaps = [(pairs[n - 1][1], pairs[n][0]) for n in range(len(pairs))]
    from_next = lax.ppermute(to_next, BOTH, gaps + [(b, a) for a, b in gaps])
    from_chip = lax.ppermute(to_chip, BOTH, pairs + [(b, a) for a, b in pairs])
    system = call(local_body, 4 * flops, shape((2, count, count), F32), spread, bins)
    flops = flops + 10 * 3 * 2 * count**3
    out = shape((peers, 2, held, values), BF16)
    shared = (spread, center)
    partial = call(chip_body, flops, out, parity, system, pulls, from_chip, *shared)
    analysis = call(
        next_body, flops, out, parity, partial, system, pulls, from_next, *shared, aliases={1: 0}
    )
    return exchange(analysis.reshape(columns, held, values))


def solution(mesh):
    in_specs = (
        P("grp", "mem", None),
        P(BOTH),
        P(BOTH, None),
        P(BOTH, None),
        P(BOTH, None),
        P(BOTH, None),
    )
    return jax.shard_map(analyse, mesh=mesh, in_specs=in_specs, out_specs=P("grp", "mem", None), check_vma=False)
```

```python
import jax
import jax.numpy as jnp
import numpy as np
from jax import lax
from jax.experimental import pallas as pl
from jax.experimental.pallas import tpu as pltpu
from jax.sharding import PartitionSpec as P


BOTH = ("grp", "mem")
HIGHEST = lax.Precision.HIGHEST
F32 = jnp.float32
BF16 = jnp.bfloat16


def direction_weights(shift_amount):
    toward_west = jnp.exp(-((shift_amount + 0.5) ** 2))
    own_weight = jnp.exp(-((shift_amount - 0.5) ** 2))
    toward_east = jnp.exp(-((1.5 - shift_amount) ** 2))
    return (toward_west, own_weight, toward_east)


def binned(observations, values):
    slot, datum, precision, offset = observations
    weights = jnp.stack(direction_weights(offset)) * precision[None]
    rows = jnp.concatenate([weights, weights * datum[None]], axis=0)
    picks = slot.astype(jnp.int32)
    chosen = (picks[:, None] == jnp.arange(values, dtype=jnp.int32)[None, :]).astype(F32)
    return jnp.dot(rows, chosen, precision=HIGHEST)


def walk():
    chips = [row * 4 + (place, 3 - place)[row % 2] for row in range(8) for place in range(4)]
    return [2 * chip + core for chip in chips for core in (0, 1)]


def two_step_factors():
    root = max(np.roots([1.0, -6.0, 9.0, -12.0]), key=np.real).real
    return (-(3.0 + root) / 4, 3.0 * root / 4), ((root - 6.0) / 4, 3.0 / root)


def halves(value):
    high = value.astype(BF16)
    return high, (value - high.astype(F32)).astype(BF16)


def product(left, right):
    (left_high, left_low), (right_high, right_low) = left, right
    rows = jnp.concatenate([left_high, left_high, left_low], axis=1)
    stacked = jnp.concatenate([right_high, right_low, right_high], axis=0)
    middle = rows.shape[0] // 2
    return jnp.concatenate(
        [jnp.dot(part, stacked, preferred_element_type=F32) for part in (rows[:middle], rows[middle:])],
        axis=0,
    )


def against(left, right):
    return lax.dot_general(left, right, (((1,), (1,)), ((), ())), preferred_element_type=F32)


def weighed(spread, center, weight, driven):
    high, low = halves(driven - weight * center)
    rows = (spread.astype(F32) * weight).astype(BF16)
    return jnp.concatenate([rows, high, low, jnp.zeros((14, rows.shape[1]), BF16)], axis=0)


def outgoing_body(parity_ref, members_ref, bins_ref, spread_ref, center_ref, chip_ref, next_ref):
    peers, _, held, values = members_ref.shape
    count = peers * held
    for column in (0, 1):
        wide = members_ref[:, column].astype(F32).reshape(count, values)
        center = jnp.sum(wide, axis=0, keepdims=True) * (1.0 / count)
        center_ref[column] = center
        spread_ref[column] = (wide - center).astype(BF16)
    parity = parity_ref[0]
    for column, sent in ((parity, next_ref), (1 - parity, chip_ref)):
        bins, spread = bins_ref[column], spread_ref[column]
        weight = jnp.where(column == 0, bins[0:1], bins[2:3])
        driven = jnp.where(column == 0, bins[3:4], bins[5:6])
        gram = against(weighed(spread, center_ref[column], weight, driven), spread)
        sent[0:count, :] = gram[0:count].astype(BF16)
        high, low = halves(gram[count : count + 1] + gram[count + 1 : count + 2])
        sent[count:, :] = jnp.concatenate([high, low, jnp.zeros((14, count), BF16)], axis=0)


def local_body(spread_ref, center_ref, bins_ref, local_ref):
    for column, other, which in ((0, 1, 0), (1, 0, 2)):
        left = [
            weighed(spread_ref[c], center_ref[c], bins_ref[c, w : w + 1], bins_ref[c, 3 + w : 4 + w])
            for c, w in ((column, 1), (other, which))
        ]
        right = [spread_ref[column], spread_ref[other]]
        local_ref[column] = against(jnp.concatenate(left, axis=1), jnp.concatenate(right, axis=1))


def analysis_of(column, local_ref, received_ref, spread_ref, center_ref, out_ref):
    peers, _, held, values = out_ref.shape
    count = peers * held
    diagonal = lax.broadcasted_iota(jnp.int32, (count, count), 0) == lax.broadcasted_iota(
        jnp.int32, (count, count), 1
    )

    def scaled_eye(value):
        return jnp.where(diagonal, value, 0.0).astype(F32)

    def two_steps(square, value):
        factors = [
            halves(square + linear * value + scaled_eye(constant))
            for linear, constant in two_step_factors()
        ]
        return halves(product(*factors))

    def stacked(*values):
        return tuple(jnp.concatenate(parts, axis=0) for parts in zip(*values))

    combined = local_ref[column] + received_ref[...].astype(F32)
    system = scaled_eye(count - 1.0) + combined[0:count]
    whole = halves(system)
    squares = jnp.sum(jnp.sum((system * system).reshape(count // 8, 8, count), axis=0), axis=(0, 1), keepdims=True)
    norm = jnp.sqrt(squares)
    scale = 1.0 / norm
    first = two_steps(product(whole, whole) * (0.25 * scale * scale), system * scale)
    value = product(whole, halves(product(first, first))) * scale
    later = halves(value)
    both = product(stacked(later, first), later)
    second = two_steps(0.25 * both[:count], value)
    three = product(stacked(second, first, halves(both[count:])), second)
    twice, inverse, carried = three[:count], three[count : 2 * count], three[2 * count :]
    root = 1.5 * inverse - 0.5 * product(halves(carried), halves(twice))
    root = root * (1.0 / jnp.sqrt(norm))
    pull = combined[count : count + 1] + combined[count + 1 : count + 2]
    inner = jnp.sum(root * pull, axis=1, keepdims=True)
    mean_weight = jnp.sum(root * inner, axis=0, keepdims=True)
    transform = ((count - 1.0) ** 0.5 * root + mean_weight).astype(BF16)
    grown = jnp.dot(transform, spread_ref[column], preferred_element_type=F32)
    analysis = center_ref[column] + grown
    out_ref[:, column] = analysis.reshape(peers, held, values).astype(BF16)


def chip_body(parity_ref, *refs):
    analysis_of(1 - parity_ref[0], *refs)


def next_body(parity_ref, done_ref, *refs):
    analysis_of(parity_ref[0], *refs)


def call(body, flops, outs, *operands, aliases=None):
    return pl.pallas_call(
        body,
        out_shape=outs,
        in_specs=[
            pl.BlockSpec(memory_space=pltpu.SMEM if operand.ndim == 1 else pltpu.VMEM)
            for operand in operands
        ],
        out_specs=jax.tree.map(lambda _: pl.BlockSpec(memory_space=pltpu.VMEM), outs),
        input_output_aliases=aliases or {},
        compiler_params=pltpu.CompilerParams(vmem_limit_bytes=24 << 20),
        cost_estimate=pl.CostEstimate(flops=flops, bytes_accessed=1 << 20, transcendentals=0),
    )(*operands)


def exchange(value):
    return lax.all_to_all(
        value, "mem", split_axis=0, concat_axis=0, tiled=True, axis_index_groups=[walk()]
    )


def analyse(background, tally, slot, datum, precision, offset):
    columns, held, values = background.shape
    peers, groups = lax.axis_size("mem"), lax.axis_size("grp")
    count = peers * held
    order = walk()
    members = exchange(background).reshape(peers, 2, held, values)
    live = jnp.arange(values, dtype=jnp.int32)[None, :] < tally[:, None]
    observations = jnp.stack(
        [slot.astype(F32), datum, precision * live.astype(F32), offset], axis=0
    )
    observations = lax.ppermute(
        observations.reshape(8, values), "mem", [(p, order[p]) for p in range(peers)]
    ).reshape(4, 2, values)
    bins = jnp.stack([binned(observations[:, c], values) for c in range(2)])
    shape = jax.ShapeDtypeStruct
    sent = shape((count + 16, count), BF16)
    flops = 2 * count * count * values
    parity = (lax.axis_index("mem") % 2).astype(jnp.int32)[None]
    spread, center, to_chip, to_next = call(
        outgoing_body,
        2 * flops,
        (
            shape((2, count, values), BF16),
            shape((2, 1, values), F32),
            sent,
            sent,
        ),
        parity,
        members,
        bins,
    )
    ring = [group * peers + place for group in range(groups) for place in order]
    pairs = [tuple(ring[n : n + 2]) for n in range(0, len(ring), 2)]
    gaps = [(pairs[n - 1][1], pairs[n][0]) for n in range(len(pairs))]
    from_next = lax.ppermute(to_next, BOTH, gaps + [(b, a) for a, b in gaps])
    from_chip = lax.ppermute(to_chip, BOTH, pairs + [(b, a) for a, b in pairs])
    local = call(
        local_body, 4 * flops, shape((2, count + 16, count), F32), spread, center, bins
    )
    flops = flops + 10 * 3 * 2 * count**3
    out = shape((peers, 2, held, values), BF16)
    shared = (spread, center)
    partial = call(chip_body, flops, out, parity, local, from_chip, *shared)
    analysis = call(
        next_body, flops, out, parity, partial, local, from_next, *shared, aliases={1: 0}
    )
    return exchange(analysis.reshape(columns, held, values))


def solution(mesh):
    in_specs = (
        P("grp", "mem", None),
        P(BOTH),
        P(BOTH, None),
        P(BOTH, None),
        P(BOTH, None),
        P(BOTH, None),
    )
    return jax.shard_map(analyse, mesh=mesh, in_specs=in_specs, out_specs=P("grp", "mem", None), check_vma=False)
```
